128 devices in a mesh: dp: 16 (over x_hi, z, core), tensor: 8 (over x_lo, y).
Axes of the slice: x: 4 (x_hi: 2, x_lo: 2; x = x_hi * 2 + x_lo), y: 4, z: 4, core: 2. Of those that a mesh axis runs over, the one named last changes fastest.
Arguments:
- tokens: bfloat16 [20480, 4096], P(('dp', 'tensor')), parts along dimension 0, may hold values from -6 to 6
- norm_gain: bfloat16 [4096], replicated, may hold values from 0.099609375 to 1.8984375
- query_weight: bfloat16 [4096, 8192], P(None, 'tensor'), may hold values from -0.09375 to 0.09375
- key_weight: bfloat16 [4096, 1024], P(None, 'tensor'), may hold values from -0.09375 to 0.09375
- value_weight: bfloat16 [4096, 1024], P(None, 'tensor'), may hold values from -0.09375 to 0.09375
- out_weight: bfloat16 [8192, 4096], P('tensor'), may hold values from -0.0625 to 0.0625
- past_cache: bfloat16 [2048, 64, 2, 1024], P('dp', None, None, 'tensor'), parts along dimension 0, may hold values from -320 to 320
- exponents: int32 [20480, 32], P('dp'), parts along dimension 0, may hold values from -11 to -7
Outputs:
- mixed: bfloat16 [20480, 4096], P(('dp', 'tensor')), parts along dimension 0
The draws below stay inside these ranges and needn't reach their ends.
There are 16 independent parts, one for each index of `dp`. The reference program is written for one: setup_inputs(seed, part) draws one part's arguments, and reference() takes and returns one part's arrays. A program takes and returns all parts, laid end to end along the dimension named above; an argument that names none is the same for every part. Nothing has to cross between parts.
All inputs are finite; a program needn't handle non-finite values.
Results may differ from the reference program's by a relative error of at most 0.012.
The reference program's roundings to bfloat16 on the way count: a program that leaves them out, or rounds other values in their place, can miss the bound.
Values may be sent and summed in bfloat16 or wider, within the bound.
No kernel may reach another device: no remote copies, remote signals or barrier semaphores. Data moves between devices by JAX's collectives and lax.ppermute only.
A program may use at most 192 MiB of HBM per device.

```python
import jax
import jax.numpy as jnp
from jax import lax

D = 4096
QH = 64
KVH = 8
HD = 128
SEQS = 128
NEW = 10
CACHE = 64
QG = 128
ROWS = 1280
N_TENSOR = 8


def draw_past_cache(key, part):
    key_base = jax.random.fold_in(key, 11)
    shape_full = (SEQS, CACHE, 2, KVH * HD)
    values_out = jnp.clip(jax.random.normal(key_base, shape_full, jnp.float32), -4.0, 4.0)
    return values_out.astype(jnp.bfloat16)


def with_ends(array, key, least, top_value):
    longest = array.shape.index(max(array.shape))
    spots = []
    for shift in (0, 1):
        where = [jax.random.randint(jax.random.fold_in(key, axis), (), 0, length) for axis, length in enumerate(array.shape)]
        where[longest] = (where[longest] + shift) % array.shape[longest]
        spots.append(tuple(where))
    return array.at[spots[0]].set(least).at[spots[1]].set(top_value)


def block_scale(rng, dims, pieces, smallest, high):
    def one(dim, blocks):
        draws = jax.random.uniform(jax.random.fold_in(jax.random.fold_in(rng, 6), dim), (blocks,), jnp.float32, smallest / len(pieces), high / len(pieces))
        return jnp.repeat(jnp.exp(draws), dims[dim] // blocks).reshape((-1,) + (1,) * (len(dims) - dim - 1))

    gain = one(*pieces[0])
    for cut in pieces[1:]:
        gain = gain * one(*cut)
    return gain


def scatter_about(own_key, shape, width, limit, pieces=(), kind=jnp.bfloat16):
    gain = block_scale(own_key, shape, pieces, -0.22, 0.18) if pieces else 1.0
    result = jax.random.normal(own_key, shape, jnp.float32) * width * gain
    return jnp.minimum(jnp.maximum(result, -limit), limit).astype(kind)


def setup_inputs(seed: int = 0, part: int = 0) -> dict:
    streams_of = jax.random.split(jax.random.key(seed), 9)
    own_keys = jax.random.split(jax.random.fold_in(streams_of[8], part), 9)
    return {
        "tokens": scatter_about(own_keys[0], (ROWS, D), 1.0, 6.0, ((0, 8),)),
        "norm_gain": jnp.clip(1.0 + 0.18 * jax.random.normal(streams_of[1], (D,), jnp.float32), 0.099609375, 1.8984375).astype(jnp.bfloat16),
        "query_weight": scatter_about(streams_of[2], (D, QH * HD), D ** -0.5, 0.09375, ((1, 8),)),
        "key_weight": scatter_about(streams_of[3], (D, KVH * HD), D ** -0.5, 0.09375, ((1, 8),)),
        "value_weight": scatter_about(streams_of[4], (D, KVH * HD), D ** -0.5, 0.09375, ((1, 8),)),
        "out_weight": scatter_about(streams_of[5], (QH * HD, D), (QH * HD) ** -0.5, 0.0625, ((0, 8),)),
        "past_cache": draw_past_cache(jax.random.fold_in(jax.random.fold_in(streams_of[8], part), 71), part),
        "exponents": with_ends(jax.random.randint(own_keys[7], (ROWS, D // QG), -11, -6), jax.random.fold_in(own_keys[7], 1), -11, (-6) - 1).astype(jnp.int32),
    }


epsilon = 1e-05
theta_base = 500000.0

def rotate(matrix, heads):
    row_count = matrix.shape[0]
    half_dim = HD // 2
    positions = (jnp.arange(row_count, dtype=jnp.int32) % NEW + CACHE).astype(jnp.float32)
    frequency = theta_base ** (-(jnp.arange(half_dim, dtype=jnp.float32) * 2.0) / HD)
    angles = positions[:, None] * frequency[None, :]
    cosine = jnp.cos(angles)[:, None, :]
    sine_part = jnp.sin(angles)[:, None, :]
    shaped = matrix.reshape(row_count, heads, 2, half_dim)
    first = shaped[:, :, 0]
    second = shaped[:, :, 1]
    turned = jnp.stack([first * cosine - second * sine_part, second * cosine + first * sine_part], 2)
    return turned.reshape(row_count, heads * HD)

def attention(query, key_new, value_new, past_cache, kv_heads):
    row_count = query.shape[0]
    seq_count = row_count // NEW
    group_size = query.shape[1] // (kv_heads * HD)
    cache_len = past_cache.shape[1]
    query_heads = query.astype(jnp.float32).reshape(seq_count, NEW, kv_heads, group_size, HD)
    new_keys = key_new.astype(jnp.float32).reshape(seq_count, NEW, kv_heads, HD)
    new_values = value_new.astype(jnp.float32).reshape(seq_count, NEW, kv_heads, HD)
    cache_keys = past_cache[:, :, 0].astype(jnp.float32).reshape(seq_count, cache_len, kv_heads, HD)
    cache_values = past_cache[:, :, 1].astype(jnp.float32).reshape(seq_count, cache_len, kv_heads, HD)
    inv_root = 1.0 / HD ** 0.5
    cache_scores = jnp.einsum('stkgd,sckd->skgtc', query_heads, cache_keys) * inv_root
    new_scores = jnp.einsum('stkgd,sukd->skgtu', query_heads, new_keys) * inv_root
    causal = jnp.arange(NEW)[:, None] >= jnp.arange(NEW)[None, :]
    new_scores = jnp.where(causal, new_scores, -1e+30)
    row_max = jnp.maximum(cache_scores.max(-1), new_scores.max(-1))[..., None]
    cache_probs = jnp.exp(cache_scores - row_max)
    new_probs = jnp.exp(new_scores - row_max)
    denominator = (cache_probs.sum(-1) + new_probs.sum(-1))[..., None]
    cache_weights = (cache_probs / denominator).astype(jnp.bfloat16).astype(jnp.float32)
    new_weights = (new_probs / denominator).astype(jnp.bfloat16).astype(jnp.float32)
    combined = jnp.einsum('skgtc,sckd->stkgd', cache_weights, cache_values)
    combined = combined + jnp.einsum('skgtu,sukd->stkgd', new_weights, new_values)
    return combined.reshape(row_count, kv_heads * group_size * HD).astype(jnp.bfloat16)

def reference(tokens, norm_gain, query_weight, key_weight, value_weight, out_weight, past_cache, exponents):
    floats = tokens.astype(jnp.float32)
    normed = floats * lax.rsqrt(lax.optimization_barrier(jnp.mean(floats * floats, axis=-1, keepdims=True)) + epsilon)
    normed = (normed * norm_gain.astype(jnp.float32)).astype(jnp.bfloat16)
    query = rotate(jnp.dot(normed, query_weight, preferred_element_type=jnp.float32), QH).astype(jnp.bfloat16)
    key_new = rotate(jnp.dot(normed, key_weight, preferred_element_type=jnp.float32), KVH).astype(jnp.bfloat16)
    value_new = jnp.dot(normed, value_weight, preferred_element_type=jnp.float32).astype(jnp.bfloat16)
    attended = attention(query, key_new, value_new, past_cache, KVH)
    row_count = tokens.shape[0]
    groups = D // QG
    shrink = jnp.exp2(-exponents.astype(jnp.float32))[..., None]
    head_cols = QH * HD // N_TENSOR
    summed = jnp.zeros((row_count, groups, QG), jnp.float32)
    for rank in range(N_TENSOR):
        partial_value = jnp.dot(attended[:, rank * head_cols:(rank + 1) * head_cols], out_weight[rank * head_cols:(rank + 1) * head_cols], preferred_element_type=jnp.float32)
        scaled = jnp.clip(partial_value.reshape(row_count, groups, QG) * shrink, -127.0, 127.0)
        summed = summed + lax.optimization_barrier(scaled.astype(jnp.bfloat16)).astype(jnp.float32)
    restore = jnp.exp2(exponents.astype(jnp.float32))[..., None]
    layer_out = floats + (summed * restore).reshape(row_count, D)
    return layer_out.astype(jnp.bfloat16)
```

```python
import jax
import jax.numpy as jnp
import numpy as np
from jax import lax
from jax.experimental import pallas as pl
from jax.experimental.pallas import tpu as pltpu
from jax.sharding import PartitionSpec as P


HD = 128
NEW = 10
CACHE = 64
HEADS = 8
PAD = 16
BLOCK = 80
CHUNK = 16
LIMIT = 20 << 20
epsilon = 1e-05
theta_base = 500000.0


VMEM = pltpu.VMEM


def hbm(x):
    return pltpu.with_memory_space_constraint(x, pltpu.HBM)


def vmem(x):
    return pltpu.with_memory_space_constraint(x, VMEM)


def norm_kernel(first, tokens, gain, out, x, g, sems):
    rows, width = out.shape
    gain_copy = pltpu.make_async_copy(gain, g, sems.at[rows // CHUNK])
    gain_copy.start()
    for i in range(rows // CHUNK):
        pltpu.make_async_copy(
            tokens.at[pl.ds(first + i * CHUNK, CHUNK)], x.at[pl.ds(i * CHUNK, CHUNK)], sems.at[i]
        ).start()
    gain_copy.wait()

    @pl.loop(0, rows // CHUNK)
    def _(i):
        span = pl.ds(pl.multiple_of(i * CHUNK, CHUNK), CHUNK)
        pltpu.make_async_copy(x.at[span], x.at[span], sems.at[i]).wait()
        floats = x[span, :].astype(jnp.float32)
        scale = lax.rsqrt(jnp.mean(floats * floats, axis=-1, keepdims=True) + epsilon)
        for c in range(width // HD):
            cols = slice(c * HD, (c + 1) * HD)
            part = x[span, cols].astype(jnp.float32) * scale * g[c : c + 1].astype(jnp.float32)
            out[span, cols] = part.astype(jnp.bfloat16)


def norm_half(tokens, gain, half):
    rows, width = tokens.shape[0] // 2, tokens.shape[1]
    anywhere = pl.BlockSpec(memory_space=pl.ANY)
    return pl.pallas_call(
        lambda *refs: norm_kernel(half * rows, *refs),
        in_specs=[anywhere] * 2,
        out_specs=pl.BlockSpec(memory_space=VMEM),
        out_shape=VMEM((rows, width), jnp.bfloat16),
        scratch_shapes=[
            VMEM((rows, width), jnp.bfloat16),
            VMEM((width // HD, HD), jnp.bfloat16),
            pltpu.SemaphoreType.DMA((rows // CHUNK + 1,)),
        ],
        compiler_params=pltpu.CompilerParams(vmem_limit_bytes=LIMIT),
    )(hbm(tokens), hbm(gain))


def rotary_tables(rows):
    half = HD // 2
    positions = (np.arange(rows) % NEW + CACHE).astype(np.float32)
    frequency = np.float32(theta_base) ** (-(np.arange(half, dtype=np.float32) * 2.0) / HD)
    angles = positions[:, None] * frequency[None, :].astype(np.float32)
    cosine = np.cos(angles).astype(np.float32)
    sine = np.sin(angles).astype(np.float32)
    return np.concatenate([cosine, cosine], 1), np.concatenate([-sine, sine], 1)


def pad_matrix(rows):
    seqs = rows // NEW
    matrix = np.zeros((seqs * PAD, rows), np.float32)
    for s in range(seqs):
        for t in range(NEW):
            matrix[s * PAD + t, s * NEW + t] = 1.0
    return matrix


def odd_matrix(rows):
    seqs = rows // NEW
    matrix = np.zeros((seqs * 2 * CACHE, rows), np.float32)
    for s in range(seqs):
        for u in range(NEW):
            matrix[s * 2 * CACHE + 2 * u + 1, s * NEW + u] = 1.0
    return matrix


def powers(exponent, sign):
    total = jnp.zeros(exponent.shape, jnp.float32)
    for e in range(7, 12):
        total = jnp.where(exponent == -e, 2.0 ** (sign * e), total)
    return total


def spread_matrix(groups, per_slab):
    matrix = np.zeros((groups // per_slab, groups, per_slab * HD), np.float32)
    for g in range(groups):
        matrix[g // per_slab, g, (g % per_slab) * HD : (g % per_slab + 1) * HD] = 1.0
    return matrix


def block_kernel(spots, sizes, *refs):
    count, blocks = len(sizes), len(spots)
    (offsets, *refs) = refs
    pieces, refs = refs[:count], refs[count:]
    (qw, kw, vw, ow, cache, exps, cos, sin, pad, unpad, odd, spread, *refs) = refs
    outs, refs = refs[:count], refs[count:]
    (kv, ex, qs, kvs, qp, op, fresh, scores, probs, att, sems) = refs
    slab, out_slab = 256, 1024
    slabs, out_slabs = qw.shape[1] // slab, ow.shape[1] // out_slab
    seqs = BLOCK // NEW
    kv_rows = seqs * 2 * CACHE
    starts = [sum(sizes[:p]) for p in range(count)]

    copies = []
    for b, (owner, first) in enumerate(spots):
        first = pl.multiple_of(offsets[owner] + first, 8)
        cache_first = pl.multiple_of(first // NEW * (2 * CACHE), 8)
        for source, target in (
            (cache.at[pl.ds(cache_first, kv_rows)], kv.at[pl.ds(b * kv_rows, kv_rows)]),
            (exps.at[pl.ds(first, BLOCK)], ex.at[pl.ds(b * BLOCK, BLOCK)]),
        ):
            copy = pltpu.make_async_copy(source, target, sems.at[len(copies)])
            copy.start()
            copies.append(copy)

    cosine = jnp.concatenate([cos[...]] * blocks, 0)
    sine = jnp.concatenate([sin[...]] * blocks, 0)

    def rotate(m):
        swapped = pltpu.roll(m, HD // 2, 1)
        return (m * cosine + swapped * sine).astype(jnp.bfloat16)

    def rows():
        return jnp.concatenate([piece[...] for piece in pieces], 0)

    y = jnp.dot(
        rows(), jnp.concatenate([kw[...], vw[...]], 1), preferred_element_type=jnp.float32
    )
    kvs[:, :HD] = rotate(y[:, :HD])
    kvs[:, HD:] = y[:, HD:].astype(jnp.bfloat16)

    @pl.loop(0, slabs)
    def _(i):
        cols = pl.ds(pl.multiple_of(i * slab, slab), slab)
        y = jnp.dot(rows(), qw[:, cols], preferred_element_type=jnp.float32)
        for h in range(slab // HD):
            qs[i, :, h * HD : (h + 1) * HD] = rotate(y[:, h * HD : (h + 1) * HD])

    for copy in copies:
        copy.wait()
    tall = HEADS * PAD
    inv_root = 1.0 / HD**0.5
    contract_last = (((1,), (1,)), ((), ()))
    lane = lax.broadcasted_iota(jnp.int32, (tall, 2 * CACHE), 1)
    step = lax.broadcasted_iota(jnp.int32, (tall, 2 * CACHE), 0) % PAD
    is_old = lane % 2 == 0
    allowed = is_old | ((lane // 2 <= step) & (lane // 2 < NEW))

    @pl.loop(0, blocks)
    def _(b):
        own = pl.ds(pl.multiple_of(b * BLOCK, BLOCK), BLOCK)
        for i in range(slabs):
            qp[i] = jnp.dot(pad[...], qs[i, own, :], preferred_element_type=jnp.float32).astype(
                jnp.bfloat16
            )
        fresh[...] = jnp.dot(odd[...], kvs[own, :], preferred_element_type=jnp.float32).astype(
            jnp.bfloat16
        )

        def pairs(s):
            first = pl.multiple_of(b * kv_rows + s * 2 * CACHE, 2 * CACHE)
            return kv[pl.ds(first, 2 * CACHE), :]

        def fresh_span(s):
            return slice(s * 2 * CACHE, (s + 1) * 2 * CACHE)

        per = slab // HD
        for s in range(seqs):
            base = s * PAD
            query = jnp.concatenate(
                [
                    qp[h // per, base : base + PAD, h % per * HD : (h % per + 1) * HD]
                    for h in range(HEADS)
                ],
                0,
            )
            span = slice(s * tall, (s + 1) * tall)
            keys = jnp.concatenate([pairs(s), fresh[fresh_span(s), :HD]], 0)
            both = lax.dot_general(query, keys, contract_last, preferred_element_type=jnp.float32)
            score = jnp.where(is_old, both[:, : 2 * CACHE], both[:, 2 * CACHE :]) * inv_root
            scores[span] = jnp.where(allowed, score, -1e30)
        for s in range(seqs):
            span = slice(s * tall, (s + 1) * tall)
            score = scores[span]
            prob = jnp.exp(score - jnp.max(score, axis=-1, keepdims=True))
            prob = prob / jnp.sum(prob, axis=-1, keepdims=True)
            rolled = jnp.where(is_old, 0.0, pltpu.roll(prob, 1, 1))
            probs[span, : 2 * CACHE] = rolled.astype(jnp.bfloat16)
            probs[span, 2 * CACHE :] = prob.astype(jnp.bfloat16)
        for s in range(seqs):
            base = s * PAD
            span = slice(s * tall, (s + 1) * tall)
            values = jnp.concatenate([pairs(s), fresh[fresh_span(s), HD:]], 0)
            got = jnp.dot(probs[span], values, preferred_element_type=jnp.float32)
            got = got.astype(jnp.bfloat16)
            for h in range(HEADS):
                op[base : base + PAD, h * HD : (h + 1) * HD] = got[h * PAD : (h + 1) * PAD]
        att[own, :] = jnp.dot(unpad[...], op[...], preferred_element_type=jnp.float32).astype(
            jnp.bfloat16
        )

    shrinks = powers(ex[...], 1).astype(jnp.bfloat16)

    @pl.loop(0, out_slabs)
    def _(i):
        cols = pl.ds(pl.multiple_of(i * out_slab, out_slab), out_slab)
        y = jnp.dot(att[...], ow[:, cols], preferred_element_type=jnp.float32)
        shrink = jnp.dot(shrinks, spread[i], preferred_element_type=jnp.float32)
        scaled = jnp.clip(y * shrink, -127.0, 127.0).astype(jnp.bfloat16)
        for p in range(count):
            outs[p][:, cols] = scaled[starts[p] : starts[p] + sizes[p]]


def block(offsets, spots, pieces, weights):
    width = pieces[0].shape[1]
    sizes = [piece.shape[0] for piece in pieces]
    count, total = len(pieces), sum(sizes)
    seqs = BLOCK // NEW
    head_cols = HEADS * HD
    slab, out_slab = 256, 1024
    cos, sin = rotary_tables(BLOCK)
    pad = pad_matrix(BLOCK)
    spread = spread_matrix(width // HD, out_slab // HD)
    smem = pl.BlockSpec(memory_space=pltpu.SMEM)
    anywhere = pl.BlockSpec(memory_space=pl.ANY)
    inside = pl.BlockSpec(memory_space=VMEM)
    flops = 2 * total * width * (head_cols + 2 * HD) + 2 * total * head_cols * width
    call = pl.pallas_call(
        lambda *refs: block_kernel(spots, sizes, *refs),
        in_specs=[smem] + [inside] * (count + 4) + [anywhere] * 2 + [inside] * 6,
        out_specs=[inside] * count,
        out_shape=[VMEM((rows, width), jnp.bfloat16) for rows in sizes],
        scratch_shapes=[
            VMEM((len(spots) * seqs * 2 * CACHE, HD), jnp.bfloat16),
            VMEM((total, width // HD), jnp.int32),
            VMEM((head_cols // slab, total, slab), jnp.bfloat16),
            VMEM((total, 2 * HD), jnp.bfloat16),
            VMEM((head_cols // slab, seqs * PAD, slab), jnp.bfloat16),
            VMEM((seqs * PAD, head_cols), jnp.bfloat16),
            VMEM((seqs * 2 * CACHE, 2 * HD), jnp.bfloat16),
            VMEM((seqs * HEADS * PAD, 2 * CACHE), jnp.float32),
            VMEM((seqs * HEADS * PAD, 4 * CACHE), jnp.bfloat16),
            VMEM((total, head_cols), jnp.bfloat16),
            pltpu.SemaphoreType.DMA((2 * len(spots),)),
        ],
        compiler_params=pltpu.CompilerParams(vmem_limit_bytes=LIMIT),
        cost_estimate=pl.CostEstimate(flops=flops, transcendentals=0, bytes_accessed=20 << 20),
    )
    return call(
        offsets,
        *[vmem(piece) for piece in pieces],
        *weights,
        jnp.asarray(cos),
        jnp.asarray(sin),
        jnp.asarray(pad, jnp.bfloat16),
        jnp.asarray(pad.T, jnp.bfloat16),
        jnp.asarray(odd_matrix(BLOCK), jnp.bfloat16),
        jnp.asarray(spread, jnp.bfloat16),
    )


def add_kernel(jobs, *refs):
    count = len(jobs)
    bases, parts, outs = refs[:count], list(refs[count:-count]), refs[-count:]
    for base, out, (first, rows, n) in zip(bases, outs, jobs):
        mine, parts = parts[:n], parts[n:]

        @pl.loop(0, rows // CHUNK)
        def _(i, base=base, out=out, first=first, mine=mine):
            here = pl.ds(pl.multiple_of(first + i * CHUNK, CHUNK), CHUNK)
            span = pl.ds(pl.multiple_of(i * CHUNK, CHUNK), CHUNK)
            total = base[here, :].astype(jnp.float32)
            for part in mine:
                total = total + part[span, :].astype(jnp.float32)
            out[here, :] = total.astype(jnp.bfloat16)


def add_rows(*jobs):
    bases = [base for base, _, _ in jobs]
    parts = [part for _, _, some in jobs for part in some]
    shapes = [(first, some[0].shape[0], len(some)) for _, first, some in jobs]
    rows, width = max(r for _, r, _ in shapes), bases[0].shape[1]
    inside = pl.BlockSpec(memory_space=VMEM)
    return pl.pallas_call(
        lambda *refs: add_kernel(shapes, *refs),
        in_specs=[inside] * (len(bases) + len(parts)),
        out_specs=[inside] * len(bases),
        out_shape=[VMEM(base.shape, jnp.bfloat16) for base in bases],
        input_output_aliases={j: j for j in range(len(bases))},
        compiler_params=pltpu.CompilerParams(vmem_limit_bytes=LIMIT),
        cost_estimate=pl.CostEstimate(
            flops=rows * width * 64 * len(bases), transcendentals=0, bytes_accessed=rows * width * 6
        ),
    )(*[vmem(x) for x in (*bases, *parts)])


def final_kernel(half, tokens, exps, *refs):
    (*parts, out, x, exponent, e, y, sems, out_sems) = refs
    parts = parts[:4]
    rows, width = parts[0].shape
    chunks = rows // CHUNK
    first = half * rows
    e_copy = pltpu.make_async_copy(exps.at[pl.ds(first, rows)], exponent, sems.at[chunks])
    e_copy.start()
    for i in range(chunks):
        pltpu.make_async_copy(
            tokens.at[pl.ds(first + i * CHUNK, CHUNK)], x.at[pl.ds(i * CHUNK, CHUNK)], sems.at[i]
        ).start()
    e_copy.wait()
    e[...] = powers(exponent[...], -1)

    def out_copy(i):
        return pltpu.make_async_copy(
            y.at[pl.ds(i * CHUNK, CHUNK)],
            out.at[pl.ds(first + i * CHUNK, CHUNK)],
            out_sems.at[i],
        )

    @pl.loop(0, chunks)
    def _(i):
        span = pl.ds(pl.multiple_of(i * CHUNK, CHUNK), CHUNK)
        pltpu.make_async_copy(x.at[span], x.at[span], sems.at[i]).wait()
        restore = e[span, :]
        for g in range(width // HD):
            cols = slice(g * HD, (g + 1) * HD)
            summed = parts[0][span, cols].astype(jnp.float32)
            for part in parts[1:]:
                summed = summed + part[span, cols].astype(jnp.float32)
            mixed = x[span, cols].astype(jnp.float32) + summed * restore[:, g : g + 1]
            y[span, cols] = mixed.astype(jnp.bfloat16)
        out_copy(i).start()

    for i in range(chunks):
        out_copy(i).wait()


def final_half(tokens, exps, parts, half, previous=None):
    rows, width = parts[0].shape
    anywhere = pl.BlockSpec(memory_space=pl.ANY)
    inputs = [hbm(tokens), hbm(exps), *[vmem(part) for part in parts]]
    specs = [anywhere] * 2 + [pl.BlockSpec(memory_space=VMEM)] * len(parts)
    aliases = {}
    if previous is not None:
        inputs.append(previous)
        specs.append(anywhere)
        aliases = {len(inputs) - 1: 0}
    return pl.pallas_call(
        lambda *refs: final_kernel(half, *refs),
        in_specs=specs,
        out_specs=anywhere,
        out_shape=pltpu.HBM(tokens.shape, jnp.bfloat16),
        input_output_aliases=aliases,
        scratch_shapes=[
            VMEM((rows, width), jnp.bfloat16),
            VMEM((rows, exps.shape[1]), jnp.int32),
            VMEM((rows, exps.shape[1]), jnp.float32),
            VMEM((rows, width), jnp.bfloat16),
            pltpu.SemaphoreType.DMA((rows // CHUNK + 1,)),
            pltpu.SemaphoreType.DMA((rows // CHUNK,)),
        ],
        compiler_params=pltpu.CompilerParams(vmem_limit_bytes=LIMIT),
        cost_estimate=pl.CostEstimate(
            flops=rows * width * 64, transcendentals=0, bytes_accessed=rows * width * 12
        ),
    )(*inputs)


OWN, A, B, C, U, V, W, Z = range(8)


def solution(mesh):
    ring = 4
    pairs = mesh.shape["tensor"] // ring
    assert pairs == 2
    cells = [(x, y) for x in range(pairs) for y in range(ring)]
    up = [(x * ring + y, x * ring + (y + 1) % ring) for x, y in cells]
    down = [(x * ring + y, x * ring + (y - 1) % ring) for x, y in cells]
    across = [(x * ring + y, (1 - x) * ring + y) for x, y in cells]

    def owners(x, y):
        steps = ((0, 0), (0, -1), (0, 1), (1, 0), (1, -1), (1, 1), (0, 2), (1, 2))
        return [(x + dx) % pairs * ring + (y + dy) % ring for dx, dy in steps]

    table = np.array([owners(x, y) for x, y in cells], np.int32)

    def move(value, where):
        return lax.ppermute(value, "tensor", where)

    def on_device(
        tokens, norm_gain, query_weight, key_weight, value_weight, out_weight, past_cache, exponents
    ):
        own_rows = tokens.shape[0]
        half = own_rows // 2
        cut0, cut1 = 3 * CHUNK, 2 * CHUNK
        index = lax.axis_index("tensor")
        offsets = lax.dynamic_index_in_dim(jnp.asarray(table * own_rows), index, 0, False)

        seqs, cached = past_cache.shape[:2]
        cache = past_cache.reshape(seqs * cached * 2, HD)
        resident = [
            vmem(weight) for weight in (query_weight, key_weight, value_weight, out_weight)
        ]
        weights = (*resident, hbm(cache), hbm(exponents))
        gain = norm_gain.reshape(-1, HD)
        own_exponents = lax.dynamic_slice_in_dim(exponents, index * own_rows, own_rows, 0)

        n0 = norm_half(tokens, gain, 0)
        a0, b0, c0 = move(n0, up), move(n0, down), move(n0, across)
        n1 = norm_half(tokens, gain, 1)
        a1, b1, c1 = move(n1, up), move(n1, down), move(n1, across)
        u0, w0, v0 = move(a0, across), move(a0, up), move(c0, down)
        v1, u1, w1 = move(b1, across), move(c1, up), move(b1, down)
        z0a, z0b = move(u0[:cut0], up), move(v0[cut0:], down)
        z1a, z1b = move(u1[:cut1], up), move(v1[cut1:], down)

        near, far = (A, B, C), (U, V, W)
        own0, own1 = block(offsets, [(OWN, 0), (OWN, half)], [n0, n1], weights)

        def spots(which, start):
            return [(w, start) for w in which]

        pa0, pb0, pc0 = block(offsets, spots(near, 0), [a0, b0, c0], weights)
        pa1, pb1, pc1 = block(offsets, spots(near, half), [a1, b1, c1], weights)
        pu0, pv0, pw0 = block(offsets, spots(far, 0), [u0, v0, w0], weights)
        pu1, pv1, pw1 = block(offsets, spots(far, half), [u1, v1, w1], weights)
        pz0a, pz0b = block(offsets, [(Z, 0)], [z0a, z0b], weights)
        pz1a, pz1b = block(offsets, [(Z, half)], [z1a, z1b], weights)

        ru0, rv0 = move(pz0a, down), move(pz0b, up)
        ru1, rv1 = move(pz1a, down), move(pz1b, up)
        pu0, pv0 = add_rows((pu0, 0, [ru0]), (pv0, cut0, [rv0]))
        fu0, fw0, fv0 = move(pu0, across), move(pw0, down), move(pv0, up)
        pu1, pv1 = add_rows((pu1, 0, [ru1]), (pv1, cut1, [rv1]))
        fv1, fu1, fw1 = move(pv1, across), move(pu1, down), move(pw1, up)
        pa0, pc0 = add_rows((pa0, 0, [fu0, fw0]), (pc0, 0, [fv0]))
        ga0, gb0, gc0 = move(pa0, down), move(pb0, up), move(pc0, across)
        pb1, pc1 = add_rows((pb1, 0, [fv1, fw1]), (pc1, 0, [fu1]))
        ga1, gb1, gc1 = move(pa1, down), move(pb1, up), move(pc1, across)
        out = final_half(tokens, own_exponents, [own0, ga0, gb0, gc0], 0)
        return final_half(tokens, own_exponents, [own1, ga1, gb1, gc1], 1, out)

    return jax.shard_map(
        on_device,
        mesh=mesh,
        in_specs=(
            P(("dp", "tensor"), None),
            P(),
            P(None, "tensor"),
            P(None, "tensor"),
            P(None, "tensor"),
            P("tensor", None),
            P("dp", None, None, "tensor"),
            P("dp", None),
        ),
        out_specs=P(("dp", "tensor"), None),
        check_vma=False,
    )
```

```python
import jax
import jax.numpy as jnp
import numpy as np
from jax import lax
from jax.experimental import pallas as pl
from jax.experimental.pallas import tpu as pltpu
from jax.sharding import PartitionSpec as P


HD = 128
NEW = 10
CACHE = 64
HEADS = 8
PAD = 16
BLOCK = 80
CHUNK = 16
LIMIT = 20 << 20
epsilon = 1e-05
theta_base = 500000.0


VMEM = pltpu.VMEM


def hbm(x):
    return pltpu.with_memory_space_constraint(x, pltpu.HBM)


def vmem(x):
    return pltpu.with_memory_space_constraint(x, VMEM)


def norm_kernel(first, tokens, gain, out, x, g, sems):
    rows, width = out.shape
    gain_copy = pltpu.make_async_copy(gain, g, sems.at[rows // CHUNK])
    gain_copy.start()
    for i in range(rows // CHUNK):
        pltpu.make_async_copy(
            tokens.at[pl.ds(first + i * CHUNK, CHUNK)], x.at[pl.ds(i * CHUNK, CHUNK)], sems.at[i]
        ).start()
    gain_copy.wait()

    @pl.loop(0, rows // CHUNK)
    def _(i):
        span = pl.ds(pl.multiple_of(i * CHUNK, CHUNK), CHUNK)
        pltpu.make_async_copy(x.at[span], x.at[span], sems.at[i]).wait()
        floats = x[span, :].astype(jnp.float32)
        scale = lax.rsqrt(jnp.mean(floats * floats, axis=-1, keepdims=True) + epsilon)
        for c in range(width // HD):
            cols = slice(c * HD, (c + 1) * HD)
            part = x[span, cols].astype(jnp.float32) * scale * g[c : c + 1].astype(jnp.float32)
            out[span, cols] = part.astype(jnp.bfloat16)


def norm_half(tokens, gain, half):
    rows, width = tokens.shape[0] // 2, tokens.shape[1]
    anywhere = pl.BlockSpec(memory_space=pl.ANY)
    return pl.pallas_call(
        lambda *refs: norm_kernel(half * rows, *refs),
        in_specs=[anywhere] * 2,
        out_specs=pl.BlockSpec(memory_space=VMEM),
        out_shape=VMEM((rows, width), jnp.bfloat16),
        scratch_shapes=[
            VMEM((rows, width), jnp.bfloat16),
            VMEM((width // HD, HD), jnp.bfloat16),
            pltpu.SemaphoreType.DMA((rows // CHUNK + 1,)),
        ],
        compiler_params=pltpu.CompilerParams(vmem_limit_bytes=LIMIT),
    )(hbm(tokens), hbm(gain))


def rotary_tables(rows):
    half = HD // 2
    positions = (np.arange(rows) % NEW + CACHE).astype(np.float32)
    frequency = np.float32(theta_base) ** (-(np.arange(half, dtype=np.float32) * 2.0) / HD)
    angles = positions[:, None] * frequency[None, :].astype(np.float32)
    cosine = np.cos(angles).astype(np.float32)
    sine = np.sin(angles).astype(np.float32)
    return np.concatenate([cosine, cosine], 1), np.concatenate([-sine, sine], 1)


def pad_matrix(rows):
    seqs = rows // NEW
    matrix = np.zeros((seqs * PAD, rows), np.float32)
    for s in range(seqs):
        for t in range(NEW):
            matrix[s * PAD + t, s * NEW + t] = 1.0
    return matrix


def odd_matrix(rows):
    seqs = rows // NEW
    matrix = np.zeros((seqs * 2 * CACHE, rows), np.float32)
    for s in range(seqs):
        for u in range(NEW):
            matrix[s * 2 * CACHE + 2 * u + 1, s * NEW + u] = 1.0
    return matrix


def powers(exponent, sign):
    total = jnp.zeros(exponent.shape, jnp.float32)
    for e in range(7, 12):
        total = jnp.where(exponent == -e, 2.0 ** (sign * e), total)
    return total


def spread_matrix(groups, per_slab):
    matrix = np.zeros((groups // per_slab, groups, per_slab * HD), np.float32)
    for g in range(groups):
        matrix[g // per_slab, g, (g % per_slab) * HD : (g % per_slab + 1) * HD] = 1.0
    return matrix


def block_kernel(spots, sizes, *refs):
    count, blocks = len(sizes), len(spots)
    (offsets, *refs) = refs
    pieces, refs = refs[:count], refs[count:]
    (qw, kw, vw, ow, cache, exps, cos, sin, pad, unpad, odd, spread, *refs) = refs
    outs, refs = refs[:count], refs[count:]
    (kv, ex, qs, kvs, qp, op, fresh, scores, probs, att, sems) = refs
    slab, out_slab = 256, 1024
    slabs, out_slabs = qw.shape[1] // slab, ow.shape[1] // out_slab
    seqs = BLOCK // NEW
    kv_rows = seqs * 2 * CACHE
    starts = [sum(sizes[:p]) for p in range(count)]

    copies = []
    for b, (owner, first) in enumerate(spots):
        first = pl.multiple_of(offsets[owner] + first, 8)
        cache_first = pl.multiple_of(first // NEW * (2 * CACHE), 8)
        for source, target in (
            (cache.at[pl.ds(cache_first, kv_rows)], kv.at[pl.ds(b * kv_rows, kv_rows)]),
            (exps.at[pl.ds(first, BLOCK)], ex.at[pl.ds(b * BLOCK, BLOCK)]),
        ):
            copy = pltpu.make_async_copy(source, target, sems.at[len(copies)])
            copy.start()
            copies.append(copy)

    cosine = jnp.concatenate([cos[...]] * blocks, 0)
    sine = jnp.concatenate([sin[...]] * blocks, 0)

    def rotate(m):
        swapped = pltpu.roll(m, HD // 2, 1)
        return (m * cosine + swapped * sine).astype(jnp.bfloat16)

    def rows():
        return jnp.concatenate([piece[...] for piece in pieces], 0)

    y = jnp.dot(
        rows(), jnp.concatenate([kw[...], vw[...]], 1), preferred_element_type=jnp.float32
    )
    kvs[:, :HD] = rotate(y[:, :HD])
    kvs[:, HD:] = y[:, HD:].astype(jnp.bfloat16)

    @pl.loop(0, slabs)
    def _(i):
        cols = pl.ds(pl.multiple_of(i * slab, slab), slab)
        y = jnp.dot(rows(), qw[:, cols], preferred_element_type=jnp.float32)
        for h in range(slab // HD):
            qs[i, :, h * HD : (h + 1) * HD] = rotate(y[:, h * HD : (h + 1) * HD])

    for copy in copies:
        copy.wait()
    tall = HEADS * PAD
    inv_root = 1.0 / HD**0.5
    contract_last = (((1,), (1,)), ((), ()))
    lane = lax.broadcasted_iota(jnp.int32, (tall, 2 * CACHE), 1)
    step = lax.broadcasted_iota(jnp.int32, (tall, 2 * CACHE), 0) % PAD
    is_old = lane % 2 == 0
    allowed = is_old | ((lane // 2 <= step) & (lane // 2 < NEW))

    @pl.loop(0, blocks)
    def _(b):
        own = pl.ds(pl.multiple_of(b * BLOCK, BLOCK), BLOCK)
        for i in range(slabs):
            qp[i] = jnp.dot(pad[...], qs[i, own, :], preferred_element_type=jnp.float32).astype(
                jnp.bfloat16
            )
        fresh[...] = jnp.dot(odd[...], kvs[own, :], preferred_element_type=jnp.float32).astype(
            jnp.bfloat16
        )

        def pairs(s):
            first = pl.multiple_of(b * kv_rows + s * 2 * CACHE, 2 * CACHE)
            return kv[pl.ds(first, 2 * CACHE), :]

        def fresh_span(s):
            return slice(s * 2 * CACHE, (s + 1) * 2 * CACHE)

        per = slab // HD
        for s in range(seqs):
            base = s * PAD
            query = jnp.concatenate(
                [
                    qp[h // per, base : base + PAD, h % per * HD : (h % per + 1) * HD]
                    for h in range(HEADS)
                ],
                0,
            )
            span = slice(s * tall, (s + 1) * tall)
            keys = jnp.concatenate([pairs(s), fresh[fresh_span(s), :HD]], 0)
            both = lax.dot_general(query, keys, contract_last, preferred_element_type=jnp.float32)
            score = jnp.where(is_old, both[:, : 2 * CACHE], both[:, 2 * CACHE :]) * inv_root
            scores[span] = jnp.where(allowed, score, -1e30)
        for s in range(seqs):
            span = slice(s * tall, (s + 1) * tall)
            score = scores[span]
            prob = jnp.exp(score - jnp.max(score, axis=-1, keepdims=True))
            prob = prob / jnp.sum(prob, axis=-1, keepdims=True)
            rolled = jnp.where(is_old, 0.0, pltpu.roll(prob, 1, 1))
            probs[span, : 2 * CACHE] = rolled.astype(jnp.bfloat16)
            probs[span, 2 * CACHE :] = prob.astype(jnp.bfloat16)
        for s in range(seqs):
            base = s * PAD
            span = slice(s * tall, (s + 1) * tall)
            values = jnp.concatenate([pairs(s), fresh[fresh_span(s), HD:]], 0)
            got = jnp.dot(probs[span], values, preferred_element_type=jnp.float32)
            got = got.astype(jnp.bfloat16)
            for h in range(HEADS):
                op[base : base + PAD, h * HD : (h + 1) * HD] = got[h * PAD : (h + 1) * PAD]
        att[own, :] = jnp.dot(unpad[...], op[...], preferred_element_type=jnp.float32).astype(
            jnp.bfloat16
        )

    shrinks = powers(ex[...], 1).astype(jnp.bfloat16)

    @pl.loop(0, out_slabs)
    def _(i):
        cols = pl.ds(pl.multiple_of(i * out_slab, out_slab), out_slab)
        y = jnp.dot(att[...], ow[:, cols], preferred_element_type=jnp.float32)
        shrink = jnp.dot(shrinks, spread[i], preferred_element_type=jnp.float32)
        scaled = jnp.clip(y * shrink, -127.0, 127.0).astype(jnp.bfloat16)
        for p in range(count):
            outs[p][:, cols] = scaled[starts[p] : starts[p] + sizes[p]]


def block(offsets, spots, pieces, weights):
    width = pieces[0].shape[1]
    sizes = [piece.shape[0] for piece in pieces]
    count, total = len(pieces), sum(sizes)
    seqs = BLOCK // NEW
    head_cols = HEADS * HD
    slab, out_slab = 256, 1024
    cos, sin = rotary_tables(BLOCK)
    pad = pad_matrix(BLOCK)
    spread = spread_matrix(width // HD, out_slab // HD)
    smem = pl.BlockSpec(memory_space=pltpu.SMEM)
    anywhere = pl.BlockSpec(memory_space=pl.ANY)
    inside = pl.BlockSpec(memory_space=VMEM)
    flops = 2 * total * width * (head_cols + 2 * HD) + 2 * total * head_cols * width
    call = pl.pallas_call(
        lambda *refs: block_kernel(spots, sizes, *refs),
        in_specs=[smem] + [inside] * (count + 4) + [anywhere] * 2 + [inside] * 6,
        out_specs=[inside] * count,
        out_shape=[VMEM((rows, width), jnp.bfloat16) for rows in sizes],
        scratch_shapes=[
            VMEM((len(spots) * seqs * 2 * CACHE, HD), jnp.bfloat16),
            VMEM((total, width // HD), jnp.int32),
            VMEM((head_cols // slab, total, slab), jnp.bfloat16),
            VMEM((total, 2 * HD), jnp.bfloat16),
            VMEM((head_cols // slab, seqs * PAD, slab), jnp.bfloat16),
            VMEM((seqs * PAD, head_cols), jnp.bfloat16),
            VMEM((seqs * 2 * CACHE, 2 * HD), jnp.bfloat16),
            VMEM((seqs * HEADS * PAD, 2 * CACHE), jnp.float32),
            VMEM((seqs * HEADS * PAD, 4 * CACHE), jnp.bfloat16),
            VMEM((total, head_cols), jnp.bfloat16),
            pltpu.SemaphoreType.DMA((2 * len(spots),)),
        ],
        compiler_params=pltpu.CompilerParams(vmem_limit_bytes=LIMIT),
        cost_estimate=pl.CostEstimate(flops=flops, transcendentals=0, bytes_accessed=20 << 20),
    )
    return call(
        offsets,
        *[vmem(piece) for piece in pieces],
        *weights,
        jnp.asarray(cos),
        jnp.asarray(sin),
        jnp.asarray(pad, jnp.bfloat16),
        jnp.asarray(pad.T, jnp.bfloat16),
        jnp.asarray(odd_matrix(BLOCK), jnp.bfloat16),
        jnp.asarray(spread, jnp.bfloat16),
    )


def warm_kernel(offsets, *refs):
    out = refs[-1]
    for i in range(out.shape[0]):
        out[i] = offsets[i]


def warm(offsets, weights):
    smem = pl.BlockSpec(memory_space=pltpu.SMEM)
    inside = pl.BlockSpec(memory_space=VMEM)
    return pl.pallas_call(
        warm_kernel,
        in_specs=[smem] + [inside] * len(weights),
        out_specs=smem,
        out_shape=jax.ShapeDtypeStruct(offsets.shape, offsets.dtype),
        compiler_params=pltpu.CompilerParams(vmem_limit_bytes=LIMIT),
        name="warm",
    )(offsets, *weights)


def add_kernel(jobs, *refs):
    count = len(jobs)
    bases, parts, outs = refs[:count], list(refs[count:-count]), refs[-count:]
    for base, out, (first, rows, n) in zip(bases, outs, jobs):
        mine, parts = parts[:n], parts[n:]

        @pl.loop(0, rows // CHUNK)
        def _(i, base=base, out=out, first=first, mine=mine):
            here = pl.ds(pl.multiple_of(first + i * CHUNK, CHUNK), CHUNK)
            span = pl.ds(pl.multiple_of(i * CHUNK, CHUNK), CHUNK)
            total = base[here, :].astype(jnp.float32)
            for part in mine:
                total = total + part[span, :].astype(jnp.float32)
            out[here, :] = total.astype(jnp.bfloat16)


def add_rows(*jobs):
    bases = [base for base, _, _ in jobs]
    parts = [part for _, _, some in jobs for part in some]
    shapes = [(first, some[0].shape[0], len(some)) for _, first, some in jobs]
    rows, width = max(r for _, r, _ in shapes), bases[0].shape[1]
    inside = pl.BlockSpec(memory_space=VMEM)
    return pl.pallas_call(
        lambda *refs: add_kernel(shapes, *refs),
        in_specs=[inside] * (len(bases) + len(parts)),
        out_specs=[inside] * len(bases),
        out_shape=[VMEM(base.shape, jnp.bfloat16) for base in bases],
        input_output_aliases={j: j for j in range(len(bases))},
        compiler_params=pltpu.CompilerParams(vmem_limit_bytes=LIMIT),
        cost_estimate=pl.CostEstimate(
            flops=rows * width * 64 * len(bases), transcendentals=0, bytes_accessed=rows * width * 6
        ),
    )(*[vmem(x) for x in (*bases, *parts)])


def final_kernel(half, offsets, tokens, exps, *refs):
    (*parts, out, x, exponent, e, y, sems, out_sems) = refs
    parts = parts[:4]
    rows, width = parts[0].shape
    chunks = rows // CHUNK
    first = half * rows
    e_copy = pltpu.make_async_copy(
        exps.at[pl.ds(pl.multiple_of(offsets[OWN] + first, 8), rows)], exponent, sems.at[chunks]
    )
    e_copy.start()
    for i in range(chunks):
        pltpu.make_async_copy(
            tokens.at[pl.ds(first + i * CHUNK, CHUNK)], x.at[pl.ds(i * CHUNK, CHUNK)], sems.at[i]
        ).start()
    e_copy.wait()
    e[...] = powers(exponent[...], -1)

    def out_copy(i):
        return pltpu.make_async_copy(
            y.at[pl.ds(i * CHUNK, CHUNK)],
            out.at[pl.ds(first + i * CHUNK, CHUNK)],
            out_sems.at[i],
        )

    @pl.loop(0, chunks)
    def _(i):
        span = pl.ds(pl.multiple_of(i * CHUNK, CHUNK), CHUNK)
        pltpu.make_async_copy(x.at[span], x.at[span], sems.at[i]).wait()
        restore = e[span, :]
        for g in range(width // HD):
            cols = slice(g * HD, (g + 1) * HD)
            summed = parts[0][span, cols].astype(jnp.float32)
            for part in parts[1:]:
                summed = summed + part[span, cols].astype(jnp.float32)
            mixed = x[span, cols].astype(jnp.float32) + summed * restore[:, g : g + 1]
            y[span, cols] = mixed.astype(jnp.bfloat16)
        out_copy(i).start()

    for i in range(chunks):
        out_copy(i).wait()


def final_half(offsets, tokens, exps, parts, half, previous=None):
    rows, width = parts[0].shape
    anywhere = pl.BlockSpec(memory_space=pl.ANY)
    inputs = [offsets, hbm(tokens), hbm(exps), *[vmem(part) for part in parts]]
    specs = [pl.BlockSpec(memory_space=pltpu.SMEM)] + [anywhere] * 2 + [pl.BlockSpec(memory_space=VMEM)] * len(parts)
    aliases = {}
    if previous is not None:
        inputs.append(previous)
        specs.append(anywhere)
        aliases = {len(inputs) - 1: 0}
    return pl.pallas_call(
        lambda *refs: final_kernel(half, *refs),
        in_specs=specs,
        out_specs=anywhere,
        out_shape=pltpu.HBM(tokens.shape, jnp.bfloat16),
        input_output_aliases=aliases,
        scratch_shapes=[
            VMEM((rows, width), jnp.bfloat16),
            VMEM((rows, exps.shape[1]), jnp.int32),
            VMEM((rows, exps.shape[1]), jnp.float32),
            VMEM((rows, width), jnp.bfloat16),
            pltpu.SemaphoreType.DMA((rows // CHUNK + 1,)),
            pltpu.SemaphoreType.DMA((rows // CHUNK,)),
        ],
        compiler_params=pltpu.CompilerParams(vmem_limit_bytes=LIMIT),
        cost_estimate=pl.CostEstimate(
            flops=rows * width * 64, transcendentals=0, bytes_accessed=rows * width * 12
        ),
    )(*inputs)


OWN, A, B, C, U, V, W, Z = range(8)


def solution(mesh):
    ring = 4
    pairs = mesh.shape["tensor"] // ring
    assert pairs == 2
    cells = [(x, y) for x in range(pairs) for y in range(ring)]
    up = [(x * ring + y, x * ring + (y + 1) % ring) for x, y in cells]
    down = [(x * ring + y, x * ring + (y - 1) % ring) for x, y in cells]
    across = [(x * ring + y, (1 - x) * ring + y) for x, y in cells]

    def owners(x, y):
        steps = ((0, 0), (0, -1), (0, 1), (1, 0), (1, -1), (1, 1), (0, 2), (1, 2))
        return [(x + dx) % pairs * ring + (y + dy) % ring for dx, dy in steps]

    table = np.array([owners(x, y) for x, y in cells], np.int32)

    def move(value, where):
        return lax.ppermute(value, "tensor", where)

    def on_device(
        tokens, norm_gain, query_weight, key_weight, value_weight, out_weight, past_cache, exponents
    ):
        own_rows = tokens.shape[0]
        half = own_rows // 2
        cut0, cut1 = 3 * CHUNK, 2 * CHUNK
        index = lax.axis_index("tensor")
        offsets = lax.dynamic_index_in_dim(jnp.asarray(table * own_rows), index, 0, False)

        seqs, cached = past_cache.shape[:2]
        cache = past_cache.reshape(seqs * cached * 2, HD)
        resident = [
            vmem(weight) for weight in (query_weight, key_weight, value_weight, out_weight)
        ]
        weights = (*resident, hbm(cache), hbm(exponents))
        offsets = warm(offsets, resident)
        gain = norm_gain.reshape(-1, HD)

        n0 = norm_half(tokens, gain, 0)
        a0, b0, c0 = move(n0, up), move(n0, down), move(n0, across)
        n1 = norm_half(tokens, gain, 1)
        a1, b1, c1 = move(n1, up), move(n1, down), move(n1, across)
        u0, w0, v0 = move(a0, across), move(a0, up), move(c0, down)
        v1, u1, w1 = move(b1, across), move(c1, up), move(b1, down)
        z0a, z0b = move(u0[:cut0], up), move(v0[cut0:], down)
        z1a, z1b = move(u1[:cut1], up), move(v1[cut1:], down)

        near, far = (A, B, C), (U, V, W)
        own0, own1 = block(offsets, [(OWN, 0), (OWN, half)], [n0, n1], weights)

        def spots(which, start):
            return [(w, start) for w in which]

        pa0, pb0, pc0 = block(offsets, spots(near, 0), [a0, b0, c0], weights)
        pa1, pb1, pc1 = block(offsets, spots(near, half), [a1, b1, c1], weights)
        pu0, pv0, pw0 = block(offsets, spots(far, 0), [u0, v0, w0], weights)
        pu1, pv1, pw1 = block(offsets, spots(far, half), [u1, v1, w1], weights)
        pz0a, pz0b = block(offsets, [(Z, 0)], [z0a, z0b], weights)
        pz1a, pz1b = block(offsets, [(Z, half)], [z1a, z1b], weights)

        ru0, rv0 = move(pz0a, down), move(pz0b, up)
        ru1, rv1 = move(pz1a, down), move(pz1b, up)
        pu0, pv0 = add_rows((pu0, 0, [ru0]), (pv0, cut0, [rv0]))
        fu0, fw0, fv0 = move(pu0, across), move(pw0, down), move(pv0, up)
        pu1, pv1 = add_rows((pu1, 0, [ru1]), (pv1, cut1, [rv1]))
        fv1, fu1, fw1 = move(pv1, across), move(pu1, down), move(pw1, up)
        pa0, pc0 = add_rows((pa0, 0, [fu0, fw0]), (pc0, 0, [fv0]))
        ga0, gb0, gc0 = move(pa0, down), move(pb0, up), move(pc0, across)
        pb1, pc1 = add_rows((pb1, 0, [fv1, fw1]), (pc1, 0, [fu1]))
        ga1, gb1, gc1 = move(pa1, down), move(pb1, up), move(pc1, across)
        out = final_half(offsets, tokens, exponents, [own0, ga0, gb0, gc0], 0)
        return final_half(offsets, tokens, exponents, [own1, ga1, gb1, gc1], 1, out)

    return jax.shard_map(
        on_device,
        mesh=mesh,
        in_specs=(
            P(("dp", "tensor"), None),
            P(),
            P(None, "tensor"),
            P(None, "tensor"),
            P(None, "tensor"),
            P("tensor", None),
            P("dp", None, None, "tensor"),
            P("dp", None),
        ),
        out_specs=P(("dp", "tensor"), None),
        check_vma=False,
    )
```

```python
import jax
import jax.numpy as jnp
import numpy as np
from jax import lax
from jax.experimental import pallas as pl
from jax.experimental.pallas import tpu as pltpu
from jax.sharding import PartitionSpec as P


HD = 128
NEW = 10
CACHE = 64
HEADS = 8
PAD = 16
BLOCK = 80
CHUNK = 16
LIMIT = 20 << 20
epsilon = 1e-05
theta_base = 500000.0


VMEM = pltpu.VMEM


def hbm(x):
    return pltpu.with_memory_space_constraint(x, pltpu.HBM)


def vmem(x):
    return pltpu.with_memory_space_constraint(x, VMEM)


def norm_kernel(first, tokens, gain, out, x, g, sems):
    rows, width = out.shape
    gain_copy = pltpu.make_async_copy(gain, g, sems.at[rows // CHUNK])
    gain_copy.start()
    for i in range(rows // CHUNK):
        pltpu.make_async_copy(
            tokens.at[pl.ds(first + i * CHUNK, CHUNK)], x.at[pl.ds(i * CHUNK, CHUNK)], sems.at[i]
        ).start()
    gain_copy.wait()

    @pl.loop(0, rows // CHUNK)
    def _(i):
        span = pl.ds(pl.multiple_of(i * CHUNK, CHUNK), CHUNK)
        pltpu.make_async_copy(x.at[span], x.at[span], sems.at[i]).wait()
        floats = x[span, :].astype(jnp.float32)
        scale = lax.rsqrt(jnp.mean(floats * floats, axis=-1, keepdims=True) + epsilon)
        for c in range(width // HD):
            cols = slice(c * HD, (c + 1) * HD)
            part = x[span, cols].astype(jnp.float32) * scale * g[c : c + 1].astype(jnp.float32)
            out[span, cols] = part.astype(jnp.bfloat16)


def norm_half(tokens, gain, half):
    rows, width = tokens.shape[0] // 2, tokens.shape[1]
    anywhere = pl.BlockSpec(memory_space=pl.ANY)
    return pl.pallas_call(
        lambda *refs: norm_kernel(half * rows, *refs),
        in_specs=[anywhere] * 2,
        out_specs=pl.BlockSpec(memory_space=VMEM),
        out_shape=VMEM((rows, width), jnp.bfloat16),
        scratch_shapes=[
            VMEM((rows, width), jnp.bfloat16),
            VMEM((width // HD, HD), jnp.bfloat16),
            pltpu.SemaphoreType.DMA((rows // CHUNK + 1,)),
        ],
        compiler_params=pltpu.CompilerParams(vmem_limit_bytes=LIMIT),
    )(hbm(tokens), hbm(gain))


def rotary_tables(rows):
    half = HD // 2
    positions = (np.arange(rows) % NEW + CACHE).astype(np.float32)
    frequency = np.float32(theta_base) ** (-(np.arange(half, dtype=np.float32) * 2.0) / HD)
    angles = positions[:, None] * frequency[None, :].astype(np.float32)
    cosine = np.cos(angles).astype(np.float32)
    sine = np.sin(angles).astype(np.float32)
    return np.concatenate([cosine, cosine], 1), np.concatenate([-sine, sine], 1)


def pad_matrix(rows):
    seqs = rows // NEW
    matrix = np.zeros((seqs * PAD, rows), np.float32)
    for s in range(seqs):
        for t in range(NEW):
            matrix[s * PAD + t, s * NEW + t] = 1.0
    return matrix


def odd_matrix(rows):
    seqs = rows // NEW
    matrix = np.zeros((seqs * 2 * PAD, rows), np.float32)
    for s in range(seqs):
        for u in range(NEW):
            matrix[s * 2 * PAD + 2 * u + 1, s * NEW + u] = 1.0
    return matrix


def powers(exponent, sign):
    total = jnp.zeros(exponent.shape, jnp.float32)
    for e in range(7, 12):
        total = jnp.where(exponent == -e, 2.0 ** (sign * e), total)
    return total


def spread_matrix(groups, per_slab):
    matrix = np.zeros((groups // per_slab, groups, per_slab * HD), np.float32)
    for g in range(groups):
        matrix[g // per_slab, g, (g % per_slab) * HD : (g % per_slab + 1) * HD] = 1.0
    return matrix


def block_kernel(spots, sizes, *refs):
    count, blocks = len(sizes), len(spots)
    (offsets, *refs) = refs
    pieces, refs = refs[:count], refs[count:]
    (qw, kw, vw, ow, cache, exps, cos, sin, pad, unpad, odd, spread, *refs) = refs
    outs, refs = refs[:count], refs[count:]
    (kv, ex, qs, kvs, qp, op, fresh, scores, probs, att, sems) = refs
    slab, out_slab = 1024, 4096
    slabs, out_slabs = qw.shape[1] // slab, ow.shape[1] // out_slab
    seqs = BLOCK // NEW
    kv_rows = seqs * 2 * CACHE
    starts = [sum(sizes[:p]) for p in range(count)]

    copies = []
    for b, (owner, first) in enumerate(spots):
        first = pl.multiple_of(offsets[owner] + first, 8)
        cache_first = pl.multiple_of(first // NEW * (2 * CACHE), 8)
        for source, target in (
            (cache.at[pl.ds(cache_first, kv_rows)], kv.at[pl.ds(b * kv_rows, kv_rows)]),
            (exps.at[pl.ds(first, BLOCK)], ex.at[pl.ds(b * BLOCK, BLOCK)]),
        ):
            copy = pltpu.make_async_copy(source, target, sems.at[len(copies)])
            copy.start()
            copies.append(copy)

    cosine = jnp.concatenate([cos[...]] * blocks, 0)
    sine = jnp.concatenate([sin[...]] * blocks, 0)

    def rotate(m):
        swapped = pltpu.roll(m, HD // 2, 1)
        return (m * cosine + swapped * sine).astype(jnp.bfloat16)

    def rows():
        return jnp.concatenate([piece[...] for piece in pieces], 0)

    y = jnp.dot(
        rows(), jnp.concatenate([kw[...], vw[...]], 1), preferred_element_type=jnp.float32
    )
    kvs[:, :HD] = rotate(y[:, :HD])
    kvs[:, HD:] = y[:, HD:].astype(jnp.bfloat16)

    @pl.loop(0, slabs)
    def _(i):
        cols = pl.ds(pl.multiple_of(i * slab, slab), slab)
        y = jnp.dot(rows(), qw[:, cols], preferred_element_type=jnp.float32)
        for h in range(slab // HD):
            qs[i, :, h * HD : (h + 1) * HD] = rotate(y[:, h * HD : (h + 1) * HD])

    for copy in copies:
        copy.wait()
    tall = HEADS * PAD
    inv_root = 1.0 / HD**0.5
    contract_last = (((1,), (1,)), ((), ()))
    lane = lax.broadcasted_iota(jnp.int32, (tall, 2 * CACHE), 1)
    step = lax.broadcasted_iota(jnp.int32, (tall, 2 * CACHE), 0) % PAD
    is_old = lane % 2 == 0
    allowed = is_old | ((lane // 2 <= step) & (lane // 2 < NEW))

    fresh[...] = jnp.zeros(fresh.shape, fresh.dtype)

    @pl.loop(0, blocks)
    def _(b):
        own = pl.ds(pl.multiple_of(b * BLOCK, BLOCK), BLOCK)
        for i in range(slabs):
            qp[i] = jnp.dot(pad[...], qs[i, own, :], preferred_element_type=jnp.float32).astype(
                jnp.bfloat16
            )
        new = jnp.dot(odd[...], kvs[own, :], preferred_element_type=jnp.float32)
        new = new.astype(jnp.bfloat16)
        for s in range(seqs):
            part = new[s * 2 * PAD : (s + 1) * 2 * PAD]
            fresh[s * 2 * CACHE : s * 2 * CACHE + 2 * PAD] = part

        def pairs(s):
            first = pl.multiple_of(b * kv_rows + s * 2 * CACHE, 2 * CACHE)
            return kv[pl.ds(first, 2 * CACHE), :]

        def fresh_span(s):
            return slice(s * 2 * CACHE, (s + 1) * 2 * CACHE)

        per = slab // HD
        for s in range(seqs):
            base = s * PAD
            query = jnp.concatenate(
                [
                    qp[h // per, base : base + PAD, h % per * HD : (h % per + 1) * HD]
                    for h in range(HEADS)
                ],
                0,
            )
            span = slice(s * tall, (s + 1) * tall)
            keys = jnp.concatenate([pairs(s), fresh[fresh_span(s), :HD]], 0)
            both = lax.dot_general(query, keys, contract_last, preferred_element_type=jnp.float32)
            score = jnp.where(is_old, both[:, : 2 * CACHE], both[:, 2 * CACHE :]) * inv_root
            scores[span] = jnp.where(allowed, score, -1e30)
        for s in range(seqs):
            span = slice(s * tall, (s + 1) * tall)
            score = scores[span]
            prob = jnp.exp(score - jnp.max(score, axis=-1, keepdims=True))
            prob = prob / jnp.sum(prob, axis=-1, keepdims=True)
            rolled = jnp.where(is_old, 0.0, pltpu.roll(prob, 1, 1))
            probs[span, : 2 * CACHE] = rolled.astype(jnp.bfloat16)
            probs[span, 2 * CACHE :] = prob[:, : 2 * PAD].astype(jnp.bfloat16)
        for s in range(seqs):
            base = s * PAD
            span = slice(s * tall, (s + 1) * tall)
            new = fresh[s * 2 * CACHE : s * 2 * CACHE + 2 * PAD, HD:]
            values = jnp.concatenate([pairs(s), new], 0)
            got = jnp.dot(probs[span], values, preferred_element_type=jnp.float32)
            got = got.astype(jnp.bfloat16)
            for h in range(HEADS):
                op[base : base + PAD, h * HD : (h + 1) * HD] = got[h * PAD : (h + 1) * PAD]
        att[own, :] = jnp.dot(unpad[...], op[...], preferred_element_type=jnp.float32).astype(
            jnp.bfloat16
        )

    shrinks = powers(ex[...], 1).astype(jnp.bfloat16)

    @pl.loop(0, out_slabs)
    def _(i):
        cols = pl.ds(pl.multiple_of(i * out_slab, out_slab), out_slab)
        y = jnp.dot(att[...], ow[:, cols], preferred_element_type=jnp.float32)
        shrink = jnp.dot(shrinks, spread[i], preferred_element_type=jnp.float32)
        scaled = jnp.clip(y * shrink, -127.0, 127.0).astype(jnp.bfloat16)
        for p in range(count):
            outs[p][:, cols] = scaled[starts[p] : starts[p] + sizes[p]]


def block(offsets, spots, pieces, weights):
    width = pieces[0].shape[1]
    sizes = [piece.shape[0] for piece in pieces]
    count, total = len(pieces), sum(sizes)
    seqs = BLOCK // NEW
    head_cols = HEADS * HD
    slab, out_slab = 1024, 4096
    cos, sin = rotary_tables(BLOCK)
    pad = pad_matrix(BLOCK)
    spread = spread_matrix(width // HD, out_slab // HD)
    smem = pl.BlockSpec(memory_space=pltpu.SMEM)
    anywhere = pl.BlockSpec(memory_space=pl.ANY)
    inside = pl.BlockSpec(memory_space=VMEM)
    flops = 2 * total * width * (head_cols + 2 * HD) + 2 * total * head_cols * width
    call = pl.pallas_call(
        lambda *refs: block_kernel(spots, sizes, *refs),
        in_specs=[smem] + [inside] * (count + 4) + [anywhere] * 2 + [inside] * 6,
        out_specs=[inside] * count,
        out_shape=[VMEM((rows, width), jnp.bfloat16) for rows in sizes],
        scratch_shapes=[
            VMEM((len(spots) * seqs * 2 * CACHE, HD), jnp.bfloat16),
            VMEM((total, width // HD), jnp.int32),
            VMEM((head_cols // slab, total, slab), jnp.bfloat16),
            VMEM((total, 2 * HD), jnp.bfloat16),
            VMEM((head_cols // slab, seqs * PAD, slab), jnp.bfloat16),
            VMEM((seqs * PAD, head_cols), jnp.bfloat16),
            VMEM((seqs * 2 * CACHE, 2 * HD), jnp.bfloat16),
            VMEM((seqs * HEADS * PAD, 2 * CACHE), jnp.float32),
            VMEM((seqs * HEADS * PAD, 2 * CACHE + 2 * PAD), jnp.bfloat16),
            VMEM((total, head_cols), jnp.bfloat16),
            pltpu.SemaphoreType.DMA((2 * len(spots),)),
        ],
        compiler_params=pltpu.CompilerParams(vmem_limit_bytes=LIMIT),
        cost_estimate=pl.CostEstimate(flops=flops, transcendentals=0, bytes_accessed=20 << 20),
    )
    return call(
        offsets,
        *[vmem(piece) for piece in pieces],
        *weights,
        jnp.asarray(cos),
        jnp.asarray(sin),
        jnp.asarray(pad, jnp.bfloat16),
        jnp.asarray(pad.T, jnp.bfloat16),
        jnp.asarray(odd_matrix(BLOCK), jnp.bfloat16),
        jnp.asarray(spread, jnp.bfloat16),
    )


def warm_kernel(offsets, *refs):
    out = refs[-1]
    for i in range(out.shape[0]):
        out[i] = offsets[i]


def warm(offsets, weights):
    smem = pl.BlockSpec(memory_space=pltpu.SMEM)
    inside = pl.BlockSpec(memory_space=VMEM)
    return pl.pallas_call(
        warm_kernel,
        in_specs=[smem] + [inside] * len(weights),
        out_specs=smem,
        out_shape=jax.ShapeDtypeStruct(offsets.shape, offsets.dtype),
        compiler_params=pltpu.CompilerParams(vmem_limit_bytes=LIMIT),
        name="warm",
    )(offsets, *weights)


def add_kernel(jobs, *refs):
    count = len(jobs)
    bases, parts, outs = refs[:count], list(refs[count:-count]), refs[-count:]
    for base, out, (first, rows, n) in zip(bases, outs, jobs):
        mine, parts = parts[:n], parts[n:]

        @pl.loop(0, rows // CHUNK)
        def _(i, base=base, out=out, first=first, mine=mine):
            here = pl.ds(pl.multiple_of(first + i * CHUNK, CHUNK), CHUNK)
            span = pl.ds(pl.multiple_of(i * CHUNK, CHUNK), CHUNK)
            total = base[here, :].astype(jnp.float32)
            for part in mine:
                total = total + part[span, :].astype(jnp.float32)
            out[here, :] = total.astype(jnp.bfloat16)


def add_rows(*jobs):
    bases = [base for base, _, _ in jobs]
    parts = [part for _, _, some in jobs for part in some]
    shapes = [(first, some[0].shape[0], len(some)) for _, first, some in jobs]
    rows, width = max(r for _, r, _ in shapes), bases[0].shape[1]
    inside = pl.BlockSpec(memory_space=VMEM)
    return pl.pallas_call(
        lambda *refs: add_kernel(shapes, *refs),
        in_specs=[inside] * (len(bases) + len(parts)),
        out_specs=[inside] * len(bases),
        out_shape=[VMEM(base.shape, jnp.bfloat16) for base in bases],
        input_output_aliases={j: j for j in range(len(bases))},
        compiler_params=pltpu.CompilerParams(vmem_limit_bytes=LIMIT),
        cost_estimate=pl.CostEstimate(
            flops=rows * width * 64 * len(bases), transcendentals=0, bytes_accessed=rows * width * 6
        ),
    )(*[vmem(x) for x in (*bases, *parts)])


def final_kernel(half, offsets, tokens, exps, *refs):
    (*parts, out, x, exponent, e, y, sems, out_sems) = refs
    parts = parts[:4]
    rows, width = parts[0].shape
    chunks = rows // CHUNK
    first = half * rows
    e_copy = pltpu.make_async_copy(
        exps.at[pl.ds(pl.multiple_of(offsets[OWN] + first, 8), rows)], exponent, sems.at[chunks]
    )
    e_copy.start()
    for i in range(chunks):
        pltpu.make_async_copy(
            tokens.at[pl.ds(first + i * CHUNK, CHUNK)], x.at[pl.ds(i * CHUNK, CHUNK)], sems.at[i]
        ).start()
    e_copy.wait()
    e[...] = powers(exponent[...], -1)

    def out_copy(i):
        return pltpu.make_async_copy(
            y.at[pl.ds(i * CHUNK, CHUNK)],
            out.at[pl.ds(first + i * CHUNK, CHUNK)],
            out_sems.at[i],
        )

    @pl.loop(0, chunks)
    def _(i):
        span = pl.ds(pl.multiple_of(i * CHUNK, CHUNK), CHUNK)
        pltpu.make_async_copy(x.at[span], x.at[span], sems.at[i]).wait()
        restore = e[span, :]
        for g in range(width // HD):
            cols = slice(g * HD, (g + 1) * HD)
            summed = parts[0][span, cols].astype(jnp.float32)
            for part in parts[1:]:
                summed = summed + part[span, cols].astype(jnp.float32)
            mixed = x[span, cols].astype(jnp.float32) + summed * restore[:, g : g + 1]
            y[span, cols] = mixed.astype(jnp.bfloat16)
        out_copy(i).start()

    for i in range(chunks):
        out_copy(i).wait()


def final_half(offsets, tokens, exps, parts, half, previous=None):
    rows, width = parts[0].shape
    anywhere = pl.BlockSpec(memory_space=pl.ANY)
    inputs = [offsets, hbm(tokens), hbm(exps), *[vmem(part) for part in parts]]
    specs = [pl.BlockSpec(memory_space=pltpu.SMEM)] + [anywhere] * 2 + [pl.BlockSpec(memory_space=VMEM)] * len(parts)
    aliases = {}
    if previous is not None:
        inputs.append(previous)
        specs.append(anywhere)
        aliases = {len(inputs) - 1: 0}
    return pl.pallas_call(
        lambda *refs: final_kernel(half, *refs),
        in_specs=specs,
        out_specs=anywhere,
        out_shape=pltpu.HBM(tokens.shape, jnp.bfloat16),
        input_output_aliases=aliases,
        scratch_shapes=[
            VMEM((rows, width), jnp.bfloat16),
            VMEM((rows, exps.shape[1]), jnp.int32),
            VMEM((rows, exps.shape[1]), jnp.float32),
            VMEM((rows, width), jnp.bfloat16),
            pltpu.SemaphoreType.DMA((rows // CHUNK + 1,)),
            pltpu.SemaphoreType.DMA((rows // CHUNK,)),
        ],
        compiler_params=pltpu.CompilerParams(vmem_limit_bytes=LIMIT),
        cost_estimate=pl.CostEstimate(
            flops=rows * width * 64, transcendentals=0, bytes_accessed=rows * width * 12
        ),
    )(*inputs)


OWN, A, B, C, U, V, W, Z = range(8)


def solution(mesh):
    ring = 4
    pairs = mesh.shape["tensor"] // ring
    assert pairs == 2
    cells = [(x, y) for x in range(pairs) for y in range(ring)]
    up = [(x * ring + y, x * ring + (y + 1) % ring) for x, y in cells]
    down = [(x * ring + y, x * ring + (y - 1) % ring) for x, y in cells]
    across = [(x * ring + y, (1 - x) * ring + y) for x, y in cells]

    def owners(x, y):
        steps = ((0, 0), (0, -1), (0, 1), (1, 0), (1, -1), (1, 1), (0, 2), (1, 2))
        return [(x + dx) % pairs * ring + (y + dy) % ring for dx, dy in steps]

    table = np.array([owners(x, y) for x, y in cells], np.int32)

    def move(value, where):
        return lax.ppermute(value, "tensor", where)

    def on_device(
        tokens, norm_gain, query_weight, key_weight, value_weight, out_weight, past_cache, exponents
    ):
        own_rows = tokens.shape[0]
        half = own_rows // 2
        cut0, cut1 = 3 * CHUNK, 2 * CHUNK
        index = lax.axis_index("tensor")
        offsets = lax.dynamic_index_in_dim(jnp.asarray(table * own_rows), index, 0, False)

        seqs, cached = past_cache.shape[:2]
        cache = past_cache.reshape(seqs * cached * 2, HD)
        resident = [
            vmem(weight) for weight in (query_weight, key_weight, value_weight, out_weight)
        ]
        weights = (*resident, hbm(cache), hbm(exponents))
        offsets = warm(offsets, resident)
        gain = norm_gain.reshape(-1, HD)

        n0 = norm_half(tokens, gain, 0)
        a0, b0, c0 = move(n0, up), move(n0, down), move(n0, across)
        n1 = norm_half(tokens, gain, 1)
        a1, b1, c1 = move(n1, up), move(n1, down), move(n1, across)
        u0, w0, v0 = move(a0, across), move(a0, up), move(c0, down)
        v1, u1, w1 = move(b1, across), move(c1, up), move(b1, down)
        z0a, z0b = move(u0[:cut0], up), move(v0[cut0:], down)
        z1a, z1b = move(u1[:cut1], up), move(v1[cut1:], down)

        near, far = (A, B, C), (U, V, W)
        own0, own1 = block(offsets, [(OWN, 0), (OWN, half)], [n0, n1], weights)

        def spots(which, start):
            return [(w, start) for w in which]

        pa0, pb0, pc0 = block(offsets, spots(near, 0), [a0, b0, c0], weights)
        pa1, pb1, pc1 = block(offsets, spots(near, half), [a1, b1, c1], weights)
        pu0, pv0, pw0 = block(offsets, spots(far, 0), [u0, v0, w0], weights)
        pu1, pv1, pw1 = block(offsets, spots(far, half), [u1, v1, w1], weights)
        pz0a, pz0b = block(offsets, [(Z, 0)], [z0a, z0b], weights)
        pz1a, pz1b = block(offsets, [(Z, half)], [z1a, z1b], weights)

        ru0, rv0 = move(pz0a, down), move(pz0b, up)
        ru1, rv1 = move(pz1a, down), move(pz1b, up)
        pu0, pv0 = add_rows((pu0, 0, [ru0]), (pv0, cut0, [rv0]))
        fu0, fw0, fv0 = move(pu0, across), move(pw0, down), move(pv0, up)
        pu1, pv1 = add_rows((pu1, 0, [ru1]), (pv1, cut1, [rv1]))
        fv1, fu1, fw1 = move(pv1, across), move(pu1, down), move(pw1, up)
        pa0, pc0 = add_rows((pa0, 0, [fu0, fw0]), (pc0, 0, [fv0]))
        ga0, gb0, gc0 = move(pa0, down), move(pb0, up), move(pc0, across)
        pb1, pc1 = add_rows((pb1, 0, [fv1, fw1]), (pc1, 0, [fu1]))
        ga1, gb1, gc1 = move(pa1, down), move(pb1, up), move(pc1, across)
        out = final_half(offsets, tokens, exponents, [own0, ga0, gb0, gc0], 0)
        return final_half(offsets, tokens, exponents, [own1, ga1, gb1, gc1], 1, out)

    return jax.shard_map(
        on_device,
        mesh=mesh,
        in_specs=(
            P(("dp", "tensor"), None),
            P(),
            P(None, "tensor"),
            P(None, "tensor"),
            P(None, "tensor"),
            P("tensor", None),
            P("dp", None, None, "tensor"),
            P("dp", None),
        ),
        out_specs=P(("dp", "tensor"), None),
        check_vma=False,
    )
```

```python
import jax
import jax.numpy as jnp
import numpy as np
from jax import lax
from jax.experimental import pallas as pl
from jax.experimental.pallas import tpu as pltpu
from jax.sharding import PartitionSpec as P


HD = 128
NEW = 10
CACHE = 64
HEADS = 8
PAD = 16
BLOCK = 80
CHUNK = 16
LIMIT = 20 << 20
epsilon = 1e-05
theta_base = 500000.0


VMEM = pltpu.VMEM


def hbm(x):
    return pltpu.with_memory_space_constraint(x, pltpu.HBM)


def vmem(x):
    return pltpu.with_memory_space_constraint(x, VMEM)


def norm_kernel(first, tokens, gain, out, x, g, sems):
    rows, width = out.shape
    gain_copy = pltpu.make_async_copy(gain, g, sems.at[rows // CHUNK])
    gain_copy.start()
    for i in range(rows // CHUNK):
        pltpu.make_async_copy(
            tokens.at[pl.ds(first + i * CHUNK, CHUNK)], x.at[pl.ds(i * CHUNK, CHUNK)], sems.at[i]
        ).start()
    gain_copy.wait()

    @pl.loop(0, rows // CHUNK)
    def _(i):
        span = pl.ds(pl.multiple_of(i * CHUNK, CHUNK), CHUNK)
        pltpu.make_async_copy(x.at[span], x.at[span], sems.at[i]).wait()
        floats = x[span, :].astype(jnp.float32)
        scale = lax.rsqrt(jnp.mean(floats * floats, axis=-1, keepdims=True) + epsilon)
        for c in range(width // HD):
            cols = slice(c * HD, (c + 1) * HD)
            part = x[span, cols].astype(jnp.float32) * scale * g[c : c + 1].astype(jnp.float32)
            out[span, cols] = part.astype(jnp.bfloat16)


def norm_half(tokens, gain, half):
    rows, width = tokens.shape[0] // 2, tokens.shape[1]
    anywhere = pl.BlockSpec(memory_space=pl.ANY)
    return pl.pallas_call(
        lambda *refs: norm_kernel(half * rows, *refs),
        in_specs=[anywhere] * 2,
        out_specs=pl.BlockSpec(memory_space=VMEM),
        out_shape=VMEM((rows, width), jnp.bfloat16),
        scratch_shapes=[
            VMEM((rows, width), jnp.bfloat16),
            VMEM((width // HD, HD), jnp.bfloat16),
            pltpu.SemaphoreType.DMA((rows // CHUNK + 1,)),
        ],
        compiler_params=pltpu.CompilerParams(vmem_limit_bytes=LIMIT),
    )(hbm(tokens), hbm(gain))


def rotary_tables(rows):
    half = HD // 2
    positions = (np.arange(rows) % NEW + CACHE).astype(np.float32)
    frequency = np.float32(theta_base) ** (-(np.arange(half, dtype=np.float32) * 2.0) / HD)
    angles = positions[:, None] * frequency[None, :].astype(np.float32)
    cosine = np.cos(angles).astype(np.float32)
    sine = np.sin(angles).astype(np.float32)
    return np.concatenate([cosine, cosine], 1), np.concatenate([-sine, sine], 1)


def pad_matrix(rows):
    seqs = rows // NEW
    matrix = np.zeros((seqs * PAD, rows), np.float32)
    for s in range(seqs):
        for t in range(NEW):
            matrix[s * PAD + t, s * NEW + t] = 1.0
    return matrix


def odd_matrix(rows):
    seqs = rows // NEW
    matrix = np.zeros((seqs * 2 * PAD, rows), np.float32)
    for s in range(seqs):
        for u in range(NEW):
            matrix[s * 2 * PAD + 2 * u + 1, s * NEW + u] = 1.0
    return matrix


def powers(exponent, sign):
    total = jnp.zeros(exponent.shape, jnp.float32)
    for e in range(7, 12):
        total = jnp.where(exponent == -e, 2.0 ** (sign * e), total)
    return total


def slab_sizes(blocks):
    return ((512, 2048), (256, 1024), (512, 1024))[blocks - 1]


def block_kernel(spots, sizes, *refs):
    count, blocks = len(sizes), len(spots)
    (offsets, *refs) = refs
    pieces, refs = refs[:count], refs[count:]
    (qw, kw, vw, ow, cache, exps, cos, sin, pad, unpad, odd, *refs) = refs
    outs, refs = refs[:count], refs[count:]
    (kv, ex, qs, kvs, qp, op, fresh, scores, probs, att, sems) = refs
    slab, out_slab = slab_sizes(blocks)
    slabs, out_slabs = qw.shape[1] // slab, ow.shape[1] // out_slab
    seqs = BLOCK // NEW
    kv_rows = seqs * 2 * CACHE
    starts = [sum(sizes[:p]) for p in range(count)]

    copies = []
    for b, (owner, first) in enumerate(spots):
        first = pl.multiple_of(offsets[owner] + first, 8)
        cache_first = pl.multiple_of(first // NEW * (2 * CACHE), 8)
        for source, target in (
            (cache.at[pl.ds(cache_first, kv_rows)], kv.at[pl.ds(b * kv_rows, kv_rows)]),
            (exps.at[pl.ds(first, BLOCK)], ex.at[pl.ds(b * BLOCK, BLOCK)]),
        ):
            copy = pltpu.make_async_copy(source, target, sems.at[len(copies)])
            copy.start()
            copies.append(copy)

    cosine = jnp.concatenate([cos[...]] * blocks, 0)
    sine = jnp.concatenate([sin[...]] * blocks, 0)

    def rotate(m):
        swapped = pltpu.roll(m, HD // 2, 1)
        return (m * cosine + swapped * sine).astype(jnp.bfloat16)

    def rows():
        return jnp.concatenate([piece[...] for piece in pieces], 0)

    y = jnp.dot(
        rows(), jnp.concatenate([kw[...], vw[...]], 1), preferred_element_type=jnp.float32
    )
    kvs[:, :HD] = rotate(y[:, :HD])
    kvs[:, HD:] = y[:, HD:].astype(jnp.bfloat16)

    @pl.loop(0, slabs)
    def _(i):
        cols = pl.ds(pl.multiple_of(i * slab, slab), slab)
        y = jnp.dot(rows(), qw[:, cols], preferred_element_type=jnp.float32)
        for h in range(slab // HD):
            qs[i, :, h * HD : (h + 1) * HD] = rotate(y[:, h * HD : (h + 1) * HD])

    for copy in copies:
        copy.wait()
    tall = HEADS * PAD
    inv_root = 1.0 / HD**0.5
    contract_last = (((1,), (1,)), ((), ()))
    lane = lax.broadcasted_iota(jnp.int32, (tall, 2 * CACHE), 1)
    step = lax.broadcasted_iota(jnp.int32, (tall, 2 * CACHE), 0) % PAD
    is_old = lane % 2 == 0
    allowed = is_old | ((lane // 2 <= step) & (lane // 2 < NEW))

    fresh[...] = jnp.zeros(fresh.shape, fresh.dtype)

    @pl.loop(0, blocks)
    def _(b):
        own = pl.ds(pl.multiple_of(b * BLOCK, BLOCK), BLOCK)
        for i in range(slabs):
            qp[i] = jnp.dot(pad[...], qs[i, own, :], preferred_element_type=jnp.float32).astype(
                jnp.bfloat16
            )
        new = jnp.dot(odd[...], kvs[own, :], preferred_element_type=jnp.float32)
        new = new.astype(jnp.bfloat16)
        for s in range(seqs):
            part = new[s * 2 * PAD : (s + 1) * 2 * PAD]
            fresh[s * 2 * CACHE : s * 2 * CACHE + 2 * PAD] = part

        def pairs(s):
            first = pl.multiple_of(b * kv_rows + s * 2 * CACHE, 2 * CACHE)
            return kv[pl.ds(first, 2 * CACHE), :]

        def fresh_span(s):
            return slice(s * 2 * CACHE, (s + 1) * 2 * CACHE)

        per = slab // HD
        for s in range(seqs):
            base = s * PAD
            query = jnp.concatenate(
                [
                    qp[h // per, base : base + PAD, h % per * HD : (h % per + 1) * HD]
                    for h in range(HEADS)
                ],
                0,
            )
            span = slice(s * tall, (s + 1) * tall)
            keys = jnp.concatenate([pairs(s), fresh[fresh_span(s), :HD]], 0)
            both = lax.dot_general(query, keys, contract_last, preferred_element_type=jnp.float32)
            score = jnp.where(is_old, both[:, : 2 * CACHE], both[:, 2 * CACHE :]) * inv_root
            scores[span] = jnp.where(allowed, score, -1e30)
        for s in range(seqs):
            span = slice(s * tall, (s + 1) * tall)
            score = scores[span]
            prob = jnp.exp(score - jnp.max(score, axis=-1, keepdims=True))
            prob = prob / jnp.sum(prob, axis=-1, keepdims=True)
            rolled = jnp.where(is_old, 0.0, pltpu.roll(prob, 1, 1))
            probs[span, : 2 * CACHE] = rolled.astype(jnp.bfloat16)
            probs[span, 2 * CACHE :] = prob[:, : 2 * PAD].astype(jnp.bfloat16)
        for s in range(seqs):
            base = s * PAD
            span = slice(s * tall, (s + 1) * tall)
            new = fresh[s * 2 * CACHE : s * 2 * CACHE + 2 * PAD, HD:]
            values = jnp.concatenate([pairs(s), new], 0)
            got = jnp.dot(probs[span], values, preferred_element_type=jnp.float32)
            got = got.astype(jnp.bfloat16)
            for h in range(HEADS):
                op[base : base + PAD, h * HD : (h + 1) * HD] = got[h * PAD : (h + 1) * PAD]
        att[own, :] = jnp.dot(unpad[...], op[...], preferred_element_type=jnp.float32).astype(
            jnp.bfloat16
        )

    shrinks = powers(ex[...], 1).astype(jnp.bfloat16)

    @pl.loop(0, out_slabs)
    def _(i):
        cols = pl.ds(pl.multiple_of(i * out_slab, out_slab), out_slab)
        y = jnp.dot(att[...], ow[:, cols], preferred_element_type=jnp.float32)
        group = lax.broadcasted_iota(jnp.int32, (ex.shape[1], out_slab), 0)
        column = lax.broadcasted_iota(jnp.int32, (ex.shape[1], out_slab), 1) + i * out_slab
        spread = (group == column // HD).astype(jnp.float32).astype(jnp.bfloat16)
        shrink = jnp.dot(shrinks, spread, preferred_element_type=jnp.float32)
        scaled = jnp.clip(y * shrink, -127.0, 127.0).astype(jnp.bfloat16)
        for p in range(count):
            outs[p][:, cols] = scaled[starts[p] : starts[p] + sizes[p]]


def block(offsets, spots, pieces, weights):
    width = pieces[0].shape[1]
    sizes = [piece.shape[0] for piece in pieces]
    count, total = len(pieces), sum(sizes)
    seqs = BLOCK // NEW
    head_cols = HEADS * HD
    slab, _ = slab_sizes(len(spots))
    cos, sin = rotary_tables(BLOCK)
    pad = pad_matrix(BLOCK)
    smem = pl.BlockSpec(memory_space=pltpu.SMEM)
    anywhere = pl.BlockSpec(memory_space=pl.ANY)
    inside = pl.BlockSpec(memory_space=VMEM)
    flops = 2 * total * width * (head_cols + 2 * HD) + 2 * total * head_cols * width
    call = pl.pallas_call(
        lambda *refs: block_kernel(spots, sizes, *refs),
        in_specs=[smem] + [inside] * (count + 4) + [anywhere] * 2 + [inside] * 5,
        out_specs=[inside] * count,
        out_shape=[VMEM((rows, width), jnp.bfloat16) for rows in sizes],
        scratch_shapes=[
            VMEM((len(spots) * seqs * 2 * CACHE, HD), jnp.bfloat16),
            VMEM((total, width // HD), jnp.int32),
            VMEM((head_cols // slab, total, slab), jnp.bfloat16),
            VMEM((total, 2 * HD), jnp.bfloat16),
            VMEM((head_cols // slab, seqs * PAD, slab), jnp.bfloat16),
            VMEM((seqs * PAD, head_cols), jnp.bfloat16),
            VMEM((seqs * 2 * CACHE, 2 * HD), jnp.bfloat16),
            VMEM((seqs * HEADS * PAD, 2 * CACHE), jnp.float32),
            VMEM((seqs * HEADS * PAD, 2 * CACHE + 2 * PAD), jnp.bfloat16),
            VMEM((total, head_cols), jnp.bfloat16),
            pltpu.SemaphoreType.DMA((2 * len(spots),)),
        ],
        compiler_params=pltpu.CompilerParams(vmem_limit_bytes=LIMIT),
        cost_estimate=pl.CostEstimate(flops=flops, transcendentals=0, bytes_accessed=20 << 20),
    )
    return call(
        offsets,
        *[vmem(piece) for piece in pieces],
        *weights,
        jnp.asarray(cos),
        jnp.asarray(sin),
        jnp.asarray(pad, jnp.bfloat16),
        jnp.asarray(pad.T, jnp.bfloat16),
        jnp.asarray(odd_matrix(BLOCK), jnp.bfloat16),
    )


def warm_kernel(offsets, *refs):
    out = refs[-1]
    for i in range(out.shape[0]):
        out[i] = offsets[i]


def warm(offsets, weights):
    smem = pl.BlockSpec(memory_space=pltpu.SMEM)
    inside = pl.BlockSpec(memory_space=VMEM)
    return pl.pallas_call(
        warm_kernel,
        in_specs=[smem] + [inside] * len(weights),
        out_specs=smem,
        out_shape=jax.ShapeDtypeStruct(offsets.shape, offsets.dtype),
        compiler_params=pltpu.CompilerParams(vmem_limit_bytes=LIMIT),
        name="warm",
    )(offsets, *weights)


def add_kernel(jobs, *refs):
    count = len(jobs)
    bases, parts, outs = refs[:count], list(refs[count:-count]), refs[-count:]
    for base, out, (first, rows, n) in zip(bases, outs, jobs):
        mine, parts = parts[:n], parts[n:]

        @pl.loop(0, rows // CHUNK)
        def _(i, base=base, out=out, first=first, mine=mine):
            here = pl.ds(pl.multiple_of(first + i * CHUNK, CHUNK), CHUNK)
            span = pl.ds(pl.multiple_of(i * CHUNK, CHUNK), CHUNK)
            total = base[here, :].astype(jnp.float32)
            for part in mine:
                total = total + part[span, :].astype(jnp.float32)
            out[here, :] = total.astype(jnp.bfloat16)


def add_rows(*jobs):
    bases = [base for base, _, _ in jobs]
    parts = [part for _, _, some in jobs for part in some]
    shapes = [(first, some[0].shape[0], len(some)) for _, first, some in jobs]
    rows, width = max(r for _, r, _ in shapes), bases[0].shape[1]
    inside = pl.BlockSpec(memory_space=VMEM)
    return pl.pallas_call(
        lambda *refs: add_kernel(shapes, *refs),
        in_specs=[inside] * (len(bases) + len(parts)),
        out_specs=[inside] * len(bases),
        out_shape=[VMEM(base.shape, jnp.bfloat16) for base in bases],
        input_output_aliases={j: j for j in range(len(bases))},
        compiler_params=pltpu.CompilerParams(vmem_limit_bytes=LIMIT),
        cost_estimate=pl.CostEstimate(
            flops=rows * width * 64 * len(bases), transcendentals=0, bytes_accessed=rows * width * 6
        ),
    )(*[vmem(x) for x in (*bases, *parts)])


def final_kernel(half, offsets, tokens, exps, *refs):
    (*parts, out, exponent, e, y, sems, out_sems) = refs
    parts = parts[:4]
    rows, width = parts[0].shape
    chunks = rows // CHUNK
    first = half * rows
    e_copy = pltpu.make_async_copy(
        exps.at[pl.ds(pl.multiple_of(offsets[OWN] + first, 8), rows)], exponent, sems.at[0]
    )
    e_copy.start()
    e_copy.wait()
    e[...] = powers(exponent[...], -1)

    def out_copy(i):
        return pltpu.make_async_copy(
            y.at[pl.ds(i * CHUNK, CHUNK)],
            out.at[pl.ds(first + i * CHUNK, CHUNK)],
            out_sems.at[i],
        )

    @pl.loop(0, chunks)
    def _(i):
        span = pl.ds(pl.multiple_of(i * CHUNK, CHUNK), CHUNK)
        mine = pl.ds(pl.multiple_of(first + i * CHUNK, CHUNK), CHUNK)
        restore = e[span, :]
        for g in range(width // HD):
            cols = slice(g * HD, (g + 1) * HD)
            summed = parts[0][span, cols].astype(jnp.float32)
            for part in parts[1:]:
                summed = summed + part[span, cols].astype(jnp.float32)
            mixed = tokens[mine, cols].astype(jnp.float32) + summed * restore[:, g : g + 1]
            y[span, cols] = mixed.astype(jnp.bfloat16)
        out_copy(i).start()

    for i in range(chunks):
        out_copy(i).wait()


def final_half(offsets, tokens, exps, parts, half, previous=None):
    rows, width = parts[0].shape
    anywhere = pl.BlockSpec(memory_space=pl.ANY)
    inputs = [offsets, vmem(tokens), hbm(exps), *[vmem(part) for part in parts]]
    specs = [pl.BlockSpec(memory_space=pltpu.SMEM), pl.BlockSpec(memory_space=VMEM), anywhere] + [pl.BlockSpec(memory_space=VMEM)] * len(parts)
    aliases = {}
    if previous is not None:
        inputs.append(previous)
        specs.append(anywhere)
        aliases = {len(inputs) - 1: 0}
    return pl.pallas_call(
        lambda *refs: final_kernel(half, *refs),
        in_specs=specs,
        out_specs=anywhere,
        out_shape=pltpu.HBM(tokens.shape, jnp.bfloat16),
        input_output_aliases=aliases,
        scratch_shapes=[
            VMEM((rows, exps.shape[1]), jnp.int32),
            VMEM((rows, exps.shape[1]), jnp.float32),
            VMEM((rows, width), jnp.bfloat16),
            pltpu.SemaphoreType.DMA((1,)),
            pltpu.SemaphoreType.DMA((rows // CHUNK,)),
        ],
        compiler_params=pltpu.CompilerParams(vmem_limit_bytes=LIMIT),
        cost_estimate=pl.CostEstimate(
            flops=rows * width * 64, transcendentals=0, bytes_accessed=rows * width * 12
        ),
    )(*inputs)


OWN, A, B, C, U, V, W, Z = range(8)


def solution(mesh):
    ring = 4
    pairs = mesh.shape["tensor"] // ring
    assert pairs == 2
    cells = [(x, y) for x in range(pairs) for y in range(ring)]
    up = [(x * ring + y, x * ring + (y + 1) % ring) for x, y in cells]
    down = [(x * ring + y, x * ring + (y - 1) % ring) for x, y in cells]
    across = [(x * ring + y, (1 - x) * ring + y) for x, y in cells]

    def owners(x, y):
        steps = ((0, 0), (0, -1), (0, 1), (1, 0), (1, -1), (1, 1), (0, 2), (1, 2))
        return [(x + dx) % pairs * ring + (y + dy) % ring for dx, dy in steps]

    table = np.array([owners(x, y) for x, y in cells], np.int32)

    def move(value, where):
        return lax.ppermute(value, "tensor", where)

    def on_device(
        tokens, norm_gain, query_weight, key_weight, value_weight, out_weight, past_cache, exponents
    ):
        own_rows = tokens.shape[0]
        half = own_rows // 2
        cut0, cut1 = 3 * CHUNK, 2 * CHUNK
        index = lax.axis_index("tensor")
        offsets = lax.dynamic_index_in_dim(jnp.asarray(table * own_rows), index, 0, False)

        seqs, cached = past_cache.shape[:2]
        cache = past_cache.reshape(seqs * cached * 2, HD)
        resident = [
            vmem(weight) for weight in (query_weight, key_weight, value_weight, out_weight)
        ]
        weights = (*resident, hbm(cache), hbm(exponents))
        offsets = warm(offsets, resident)
        gain = norm_gain.reshape(-1, HD)

        n0 = norm_half(tokens, gain, 0)
        a0, b0, c0 = move(n0, up), move(n0, down), move(n0, across)
        n1 = norm_half(tokens, gain, 1)
        a1, b1, c1 = move(n1, up), move(n1, down), move(n1, across)
        u0, w0, v0 = move(a0, across), move(a0, up), move(c0, down)
        v1, u1, w1 = move(b1, across), move(c1, up), move(b1, down)
        z0a, z0b = move(u0[:cut0], up), move(v0[cut0:], down)
        z1a, z1b = move(u1[:cut1], up), move(v1[cut1:], down)

        near, far = (A, B, C), (U, V, W)
        own0, own1 = block(offsets, [(OWN, 0), (OWN, half)], [n0, n1], weights)

        def spots(which, start):
            return [(w, start) for w in which]

        pa0, pb0, pc0 = block(offsets, spots(near, 0), [a0, b0, c0], weights)
        pa1, pb1, pc1 = block(offsets, spots(near, half), [a1, b1, c1], weights)
        pu0, pv0, pw0 = block(offsets, spots(far, 0), [u0, v0, w0], weights)
        pu1, pv1, pw1 = block(offsets, spots(far, half), [u1, v1, w1], weights)
        pz0a, pz0b = block(offsets, [(Z, 0)], [z0a, z0b], weights)
        pz1a, pz1b = block(offsets, [(Z, half)], [z1a, z1b], weights)

        ru0, rv0 = move(pz0a, down), move(pz0b, up)
        ru1, rv1 = move(pz1a, down), move(pz1b, up)
        pu0, pv0 = add_rows((pu0, 0, [ru0]), (pv0, cut0, [rv0]))
        fu0, fw0, fv0 = move(pu0, across), move(pw0, down), move(pv0, up)
        pu1, pv1 = add_rows((pu1, 0, [ru1]), (pv1, cut1, [rv1]))
        fv1, fu1, fw1 = move(pv1, across), move(pu1, down), move(pw1, up)
        pa0, pc0 = add_rows((pa0, 0, [fu0, fw0]), (pc0, 0, [fv0]))
        ga0, gb0, gc0 = move(pa0, down), move(pb0, up), move(pc0, across)
        pb1, pc1 = add_rows((pb1, 0, [fv1, fw1]), (pc1, 0, [fu1]))
        ga1, gb1, gc1 = move(pa1, down), move(pb1, up), move(pc1, across)
        out = final_half(offsets, tokens, exponents, [own0, ga0, gb0, gc0], 0)
        return final_half(offsets, tokens, exponents, [own1, ga1, gb1, gc1], 1, out)

    return jax.shard_map(
        on_device,
        mesh=mesh,
        in_specs=(
            P(("dp", "tensor"), None),
            P(),
            P(None, "tensor"),
            P(None, "tensor"),
            P(None, "tensor"),
            P("tensor", None),
            P("dp", None, None, "tensor"),
            P("dp", None),
        ),
        out_specs=P(("dp", "tensor"), None),
        check_vma=False,
    )
```
